512 devices in a mesh: expert: 64 (over x, z), tensor: 8 (over y, core).
Axes of the slice: x: 4, y: 4, z: 16, core: 2. Of those that a mesh axis runs over, the one named last changes fastest.
Arguments:
- grad_out: bfloat16 [1024, 3584], P('expert'), may hold values from -1.5 to 1.5
- expert_ids: int32 [1024, 8], P('expert'), may hold values from 0 to 63, all different within a row; in each aligned block of 16 rows (0 to 15, 16 to 31, ...) at most 4 rows name the same one
- gate_values: float32 [1024, 8], P('expert'), may hold values from 0.05 to 0.6
- w_gate_up: bfloat16 [64, 2, 3584, 1024], P('expert', None, None, 'tensor'), may hold values from -0.09375 to 0.09375
- w_down: bfloat16 [64, 1024, 3584], P('expert', 'tensor'), may hold values from -0.1875 to 0.1875
- saved_routed: bfloat16 [64, 2, 256, 1024], P('expert', None, None, 'tensor'), may hold values from -6 to 6
- shared_gate_up: bfloat16 [2, 3584, 1024], P(None, 'expert', 'tensor'), may hold values from -0.09375 to 0.09375
- shared_down: bfloat16 [1024, 3584], P('tensor', 'expert'), may hold values from -0.1875 to 0.1875
- saved_shared: bfloat16 [2, 1024, 1024], P(None, 'expert', 'tensor'), may hold values from -6 to 6
Outputs:
- grad_in: bfloat16 [1024, 3584], P('expert', 'tensor')
- grad_gates: float32 [1024, 8], P('expert')
The draws below stay inside these ranges and needn't reach their ends.
Inputs may be any that keep to these rules, and one draw needn't show every extreme that they name: `expert_ids`: each row names 8 different experts. Among the 16 rows of one index of expert (aligned blocks of rows), no expert is named by more than 4 rows, and in some block one expert is named by exactly 4 rows.
All inputs are finite; a program needn't handle non-finite values.
Results may differ from the reference program's by a relative error of at most 0.015.
Values may be sent and summed in bfloat16 or wider, within the bound.
No kernel may reach another device: no remote copies, remote signals or barrier semaphores. Data moves between devices by JAX's collectives and lax.ppermute only.
A program may use at most 64 MiB of HBM per device.

```python
import math
import jax
import jax.numpy as jnp
import numpy as np
from jax import lax

D = 3584
FF = 1024
FF_SH = 1024
TOP = 8
TOK_DEV = 16
EXPERTS = 64
CAP = 4
SLOTS = 256
TOKENS = 1024
N_EXPERT = 64
N_TENSOR = 8


def block_scale(own_key, extent, shards, smallest, largest):
    factor_of = 1.0
    for dim, parts in shards:
        heights = jax.random.uniform(jax.random.fold_in(jax.random.fold_in(own_key, 6), dim), (parts,), jnp.float32, smallest / len(shards), largest / len(shards))
        factor_of = factor_of * jnp.repeat(jnp.exp(heights), extent[dim] // parts).reshape((-1,) + (1,) * (len(extent) - 1 - dim))
    return factor_of


def deal_out(rng, own, number, rows, count, top, bound, slope):
    ranking = jax.random.permutation(rng, count)
    crowded, usual = shares(count, rows * top, bound, slope, True), shares(count, rows * top, bound, slope, False)
    places = jnp.arange(count)

    def named(lengths, rotation):
        used = int((lengths > 0).sum())
        fixed = max(1, used // 4)
        passed = fixed + (places - fixed + rotation * (used - fixed)) % max(1, count - fixed)
        return jnp.zeros((count,), jnp.int32).at[ranking[jnp.where(places < fixed, places, passed)]].set(jnp.asarray(lengths, jnp.int32))

    lengths = jnp.where(number % 4 == 0, named(crowded, number // 4), named(usual, number - number // 4 - 1))
    mixed = jax.random.permutation(jax.random.fold_in(own, 3), count)
    donor, taker = mixed[0:count // 2 * 2:2], mixed[1:count // 2 * 2:2]
    room = jnp.minimum(lengths[donor] - 1, bound - lengths[taker]) // 2
    room = jnp.where((donor == ranking[0]) | (taker == ranking[0]) | (lengths[taker] == 0), 0, jnp.maximum(room, 0))
    passed = jax.random.randint(jax.random.fold_in(own, 4), (count // 2,), 0, 1 << 20) % (room + 1)
    lengths = lengths.at[donor].add(-passed).at[taker].add(passed)
    items = jnp.searchsorted(jnp.cumsum(lengths), jnp.arange(rows * top), side="right").astype(jnp.int32)
    table = items.reshape(top, rows).T
    table = table[jax.random.permutation(jax.random.fold_in(own, 1), rows)]
    rotation = jax.random.randint(jax.random.fold_in(own, 2), (rows, 1), 0, top)
    return jnp.take_along_axis(table, (jnp.arange(top)[None, :] + rotation) % top, axis=1)


def shares(count, total, reach, lean, full):
    weights = [(1 << 20) // math.isqrt(grade ** lean) + 1 for grade in range(1, count + 1)]
    largest = reach if full else min(reach, max(-(-total // count), total * weights[0] // sum(weights)))
    least = 1 if total - largest >= count - 1 else 0
    counts, rest = [largest] + [least] * (count - 1), total - largest - least * (count - 1)
    while rest > 0:
        candidates = [i for i in range(1, count) if counts[i] < largest] or [i for i in range(1, count) if counts[i] < reach]
        mass, left = sum([weights[i] for i in candidates]), rest
        for i in candidates:
            extra = min(reach - counts[i], max(1, left * weights[i] // mass), rest)
            counts[i] = counts[i] + extra
            rest = rest - extra
    return np.array(counts)


def scatter_about(rng, shape, width, limit, pieces=(), kind=jnp.bfloat16):
    entries = jax.random.normal(rng, shape, jnp.float32) * width
    if len(pieces) > 0:
        entries = block_scale(rng, shape, pieces, -0.22, 0.18) * entries
    return jnp.clip(entries, min=-limit, max=limit).astype(kind)


def setup_inputs(seed: int = 0) -> dict:
    key_of = jax.random.split(jax.random.key(seed), 10)
    grad_out = scatter_about(key_of[0], (TOKENS, D), 0.25, 1.5, ((0, 64),))
    expert_ids_keys = jax.random.split(jax.random.fold_in(key_of[1], 1), TOKENS // TOK_DEV)
    expert_ids_turns = jax.random.permutation(jax.random.fold_in(key_of[1], 3), TOKENS // TOK_DEV)
    expert_ids = jax.vmap(lambda own, number: deal_out(jax.random.fold_in(key_of[1], 2), own, number, TOK_DEV, EXPERTS, TOP, CAP, 2))(expert_ids_keys, expert_ids_turns).reshape((TOKENS, TOP))
    gate_values = jnp.clip(jnp.exp(math.log(0.6) - 2.4849067 * jax.random.uniform(key_of[2], (TOKENS, TOP), jnp.float32) ** block_scale(key_of[2], (TOKENS, TOP), ((0, 64),), -0.2, 0.2)), 0.05, 0.6)
    w_gate_up = scatter_about(key_of[3], (EXPERTS, 2, D, FF), D ** -0.5, 0.09375, ((0, 64), (3, 8)))
    w_down = scatter_about(key_of[4], (EXPERTS, FF, D), FF ** -0.5, 0.1875, ((0, 64), (1, 8)))
    saved_routed = scatter_about(key_of[5], (EXPERTS, 2, SLOTS, FF), 1.0, 6.0, ((0, 64), (3, 8)))
    shared_gate_up = scatter_about(key_of[6], (2, D, FF_SH), D ** -0.5, 0.09375, ((1, 64), (2, 8)))
    shared_down = scatter_about(key_of[7], (FF_SH, D), FF_SH ** -0.5, 0.1875, ((0, 8), (1, 64)))
    saved_shared = scatter_about(key_of[8], (2, TOKENS, FF_SH), 1.0, 6.0, ((1, 64), (2, 8)))
    return {"grad_out": grad_out, "expert_ids": expert_ids, "gate_values": gate_values, "w_gate_up": w_gate_up, "w_down": w_down, "saved_routed": saved_routed, "shared_gate_up": shared_gate_up, "shared_down": shared_down, "saved_shared": saved_shared}


def swiglu_grads(back_grad, saved_gate, saved_up):
    pre_gate = saved_gate.astype(jnp.float32)
    pre_up = saved_up.astype(jnp.float32)
    sigmoid = jax.nn.sigmoid(pre_gate)
    grad_gate = (back_grad * pre_up * sigmoid * (1.0 + pre_gate * (1.0 - sigmoid))).astype(jnp.bfloat16)
    grad_up = (back_grad * pre_gate * sigmoid).astype(jnp.bfloat16)
    return grad_gate, grad_up


def gate_mixture(back_grad, saved_gate, saved_up):
    pre_gate = saved_gate.astype(jnp.float32)
    pre_up = saved_up.astype(jnp.float32)
    sigmoid = jax.nn.sigmoid(pre_gate)
    return back_grad * pre_gate * sigmoid * pre_up


def slot_numbers(expert_ids):
    blocks = expert_ids.reshape(N_EXPERT, TOK_DEV * TOP).astype(jnp.int32)
    onehot = (blocks[:, :, None] == jnp.arange(EXPERTS, dtype=jnp.int32)[None, None, :]).astype(jnp.int32)
    earlier = (jnp.cumsum(onehot, axis=1) - onehot).astype(jnp.int32)
    position = jnp.sum(earlier * onehot, axis=2).astype(jnp.int32)
    offsets = jnp.arange(N_EXPERT, dtype=jnp.int32)[:, None] * CAP
    return (offsets + position).reshape(-1).astype(jnp.int32)


def reference(grad_out, expert_ids, gate_values, w_gate_up, w_down, saved_routed, shared_gate_up, shared_down, saved_shared):
    slot_flat = slot_numbers(expert_ids)
    ids_flat = expert_ids.reshape(-1).astype(jnp.int32)
    pair_token = (jnp.arange(TOKENS * TOP, dtype=jnp.int32) // TOP).astype(jnp.int32)
    source_table = jnp.full((EXPERTS, SLOTS), TOKENS, jnp.int32).at[ids_flat, slot_flat].set(pair_token)
    gate_table = jnp.zeros((EXPERTS, SLOTS), jnp.float32).at[ids_flat, slot_flat].set(gate_values.reshape(-1).astype(jnp.float32))
    padded = jnp.concatenate([grad_out, jnp.zeros((1, D), grad_out.dtype)], axis=0)
    slice_width = FF // N_TENSOR

    def one_expert(running, inputs):
        weights_gu, weights_down, saved_pre, source_row, gate_row = inputs
        slot_rows = padded[source_row]
        back_grad = jnp.dot(slot_rows, weights_down.T, preferred_element_type=jnp.float32)
        grad_gate, grad_up = swiglu_grads(back_grad, saved_pre[0], saved_pre[1])
        gate_mix = gate_mixture(back_grad, saved_pre[0], saved_pre[1])
        row_sum = jnp.zeros((SLOTS, D), jnp.float32)
        gate_sum = jnp.zeros((SLOTS,), jnp.float32)
        for slice_index in range(N_TENSOR):
            lower_edge = slice_index * slice_width
            upper_edge = lower_edge + slice_width
            slice_term = jnp.dot(grad_gate[:, lower_edge:upper_edge], weights_gu[0][:, lower_edge:upper_edge].T, preferred_element_type=jnp.float32)
            slice_term = slice_term + jnp.dot(grad_up[:, lower_edge:upper_edge], weights_gu[1][:, lower_edge:upper_edge].T, preferred_element_type=jnp.float32)
            slice_term = lax.optimization_barrier(slice_term.astype(jnp.bfloat16))
            row_sum = row_sum + slice_term.astype(jnp.float32)
            gate_piece = lax.optimization_barrier(jnp.sum(gate_mix[:, lower_edge:upper_edge], axis=1).astype(jnp.bfloat16))
            gate_sum = gate_sum + gate_piece.astype(jnp.float32)
        running = running.at[source_row].add(gate_row[:, None] * row_sum)
        return running, gate_sum

    initial = jnp.zeros((TOKENS + 1, D), jnp.float32)
    routed, gate_sums = lax.scan(one_expert, initial, (w_gate_up, w_down, saved_routed, source_table, gate_table))
    grad_gates = gate_sums[ids_flat, slot_flat].reshape(TOKENS, TOP)
    shared_back = jnp.dot(grad_out, shared_down.T, preferred_element_type=jnp.float32)
    shared_gate, shared_up = swiglu_grads(shared_back, saved_shared[0], saved_shared[1])
    shared_term = jnp.dot(shared_gate, shared_gate_up[0].T, preferred_element_type=jnp.float32)
    shared_term = shared_term + jnp.dot(shared_up, shared_gate_up[1].T, preferred_element_type=jnp.float32)
    grad_in = (routed[:TOKENS] + shared_term).astype(jnp.bfloat16)
    return grad_in, grad_gates
```

```python
import jax
import jax.numpy as jnp
from jax import lax
from jax.sharding import Mesh
from jax.sharding import PartitionSpec as P

OWNER = ("x", "z")
PARTS = ("y", "core")
F32 = jnp.float32
BF16 = jnp.bfloat16


def exchange(array, axis):
    return lax.all_to_all(array, axis, 0, 0, tiled=True)


def from_everyone(array, axis):
    peers = lax.axis_size(axis)
    return exchange(jnp.broadcast_to(array[None], (peers, *array.shape)), axis)


def contract_last(left, right):
    return lax.dot_general(left, right, (((1,), (1,)), ((), ())), preferred_element_type=F32)


def swiglu_grads(back_grad, saved_gate, saved_up):
    pre_gate = saved_gate.astype(F32)
    pre_up = saved_up.astype(F32)
    sigmoid = jax.nn.sigmoid(pre_gate)
    grad_gate = (back_grad * pre_up * sigmoid * (1.0 + pre_gate * (1.0 - sigmoid))).astype(BF16)
    grad_up = (back_grad * pre_gate * sigmoid).astype(BF16)
    return grad_gate, grad_up


def per_device(
    grad_out,
    expert_ids,
    gate_values,
    w_gate_up,
    w_down,
    saved_routed,
    shared_gate_up,
    shared_down,
    saved_shared,
):
    experts = lax.axis_size(OWNER)
    ys = lax.axis_size("y")
    parts = lax.axis_size(PARTS)
    tokens, features = grad_out.shape
    choose = expert_ids.shape[1]
    slots = saved_routed.shape[2]
    hidden = w_down.shape[1]
    capacity = slots // experts
    share = features // parts
    core = lax.axis_index("core")
    part = lax.axis_index(PARTS)
    swap = [(0, 1), (1, 0)]

    slot = jnp.arange(slots, dtype=jnp.int32)
    hit = expert_ids.T[:, None, :] == (slot // capacity)[None, :, None]
    chosen = jnp.any(hit, axis=0)
    earlier = jnp.arange(tokens)[:, None] < jnp.arange(tokens)[None, :]
    before = jnp.dot(chosen.astype(BF16), earlier.astype(BF16), preferred_element_type=F32)
    source = chosen & (before.astype(jnp.int32) == (slot % capacity)[:, None])
    columns = lax.dynamic_slice_in_dim(grad_out, part * share, share, 1)
    send = jnp.dot(source.astype(BF16), columns, preferred_element_type=F32).astype(BF16)
    own_rows = exchange(send.reshape(experts, capacity, share), OWNER).reshape(slots, share)

    piece = jnp.concatenate([shared_gate_up, shared_down.T[None]], axis=0)
    pieces = from_everyone(from_everyone(piece, "z"), "x")
    pieces = pieces.reshape(experts, 3, -1, hidden)
    down_all = pieces[:, 2].reshape(features, hidden)
    gate_all = pieces[:, 0].reshape(features, hidden)
    up_all = pieces[:, 1].reshape(features, hidden)

    down = exchange(w_down[0].reshape(hidden, ys, 2 * share).transpose(1, 0, 2), "y")
    other_rows = lax.ppermute(own_rows, "core", swap)
    low = jnp.where(core == 0, own_rows, other_rows)
    high = jnp.where(core == 0, other_rows, own_rows)
    rows = jnp.concatenate([low, high], axis=1)
    back_part = lax.dot_general(
        down, rows, (((2,), (1,)), ((), ())), preferred_element_type=F32
    ).transpose(0, 2, 1)
    back_grad = jnp.sum(exchange(back_part.astype(BF16), "y").astype(F32), axis=0)

    pre_gate, pre_up = saved_routed[0, 0], saved_routed[0, 1]
    grad_gate, grad_up = swiglu_grads(back_grad, pre_gate, pre_up)
    sigmoid = jax.nn.sigmoid(pre_gate.astype(F32))
    gate_mix = back_grad * pre_gate.astype(F32) * sigmoid * pre_up.astype(F32)
    gate_terms = jnp.sum(gate_mix, axis=1, keepdims=True).astype(BF16)

    halves = w_gate_up[0].reshape(2, ys, 2, share, hidden)
    own_half = lax.dynamic_index_in_dim(halves, core, 2, keepdims=False)
    other_half = lax.ppermute(
        lax.dynamic_index_in_dim(halves, 1 - core, 2, keepdims=False), "core", swap
    )
    mine = jnp.concatenate([grad_gate, grad_up, jnp.pad(gate_terms, ((0, 0), (0, 127)))], axis=1)
    theirs = lax.ppermute(mine, "core", swap)

    def rows_from(grads, half):
        total = 0.0
        for g in range(2):
            total = total + lax.dot_general(
                grads[:, g * hidden : (g + 1) * hidden],
                half[g],
                (((1,), (2,)), ((), ())),
                preferred_element_type=F32,
            )
        return total

    row_part = (rows_from(mine, own_half) + rows_from(theirs, other_half)).transpose(1, 0, 2)
    gates = jnp.concatenate([gate_terms, theirs[:, 2 * hidden : 2 * hidden + 1]], axis=1)
    row_part = jnp.concatenate(
        [row_part.astype(BF16), jnp.broadcast_to(gates[None], (ys, slots, 2))], axis=2
    )
    summed = jnp.sum(exchange(row_part, "y").astype(F32), axis=0)
    gate_sum = jnp.sum(summed[:, share:], axis=1, keepdims=True)
    gate_high = gate_sum.astype(BF16)
    gate_low = (gate_sum - gate_high.astype(F32)).astype(BF16)
    finished = jnp.concatenate([summed[:, :share].astype(BF16), gate_high, gate_low], axis=1)
    returned = exchange(finished.reshape(experts, capacity, share + 2), OWNER)

    shared_back = jnp.dot(grad_out, down_all, preferred_element_type=F32)
    shared_gate, shared_up = swiglu_grads(shared_back, saved_shared[0], saved_shared[1])
    shared_term = contract_last(shared_gate, gate_all) + contract_last(shared_up, up_all)
    shared_parts = shared_term.astype(BF16).reshape(tokens, parts, share).transpose(1, 0, 2)
    shared_sum = jnp.sum(exchange(shared_parts, PARTS).astype(F32), axis=0)

    pick = (hit & source[None]).transpose(0, 2, 1).reshape(choose * tokens, slots)
    picked = jnp.dot(
        pick.astype(BF16), returned.reshape(slots, share + 2), preferred_element_type=F32
    ).reshape(choose, tokens, share + 2)
    routed = jnp.sum(picked[:, :, :share] * gate_values.T[:, :, None], axis=0)
    grad_gates = jnp.sum(picked[:, :, share:], axis=2).T
    return (routed + shared_sum).astype(BF16), grad_gates


def solution(mesh):
    finer = Mesh(mesh.devices.reshape(4, 16, 4, 2), ("x", "z", "y", "core"))
    placed = (
        P(OWNER, None),
        P(OWNER, None),
        P(OWNER, None),
        P(OWNER, None, None, PARTS),
        P(OWNER, PARTS, None),
        P(OWNER, None, None, PARTS),
        P(None, OWNER, PARTS),
        P(PARTS, OWNER),
        P(None, OWNER, PARTS),
    )
    return jax.shard_map(
        per_device,
        mesh=finer,
        in_specs=placed,
        out_specs=(P(OWNER, PARTS), P(OWNER, None)),
        check_vma=False,
    )
```

```python
import jax
import jax.numpy as jnp
from jax import lax
from jax.experimental import pallas as pl
from jax.experimental.pallas import tpu as pltpu
from jax.sharding import Mesh
from jax.sharding import PartitionSpec as P

OWNER = ("x", "z")
PARTS = ("y", "core")
F32 = jnp.float32
BF16 = jnp.bfloat16
LANES = 128


def exchange(array, axis):
    return lax.all_to_all(array, axis, 0, 0, tiled=True)


def from_everyone(array, axis):
    peers = lax.axis_size(axis)
    return exchange(jnp.broadcast_to(array[None], (peers, *array.shape)), axis)


def contract_last(left, right):
    return lax.dot_general(left, right, (((1,), (1,)), ((), ())), preferred_element_type=F32)


def swiglu_grads(back_grad, saved_gate, saved_up):
    pre_gate = saved_gate.astype(F32)
    pre_up = saved_up.astype(F32)
    sigmoid = jax.nn.sigmoid(pre_gate)
    grad_gate = (back_grad * pre_up * sigmoid * (1.0 + pre_gate * (1.0 - sigmoid))).astype(BF16)
    grad_up = (back_grad * pre_gate * sigmoid).astype(BF16)
    return grad_gate, grad_up


def kernel_call(body, out_shape, scalars, *arrays):
    smem = pl.BlockSpec(memory_space=pltpu.SMEM)
    vmem = pl.BlockSpec(memory_space=pltpu.VMEM)
    return pl.pallas_call(
        body,
        out_shape=out_shape,
        in_specs=[smem] + [vmem] * len(arrays),
        out_specs=vmem,
    )(scalars, *arrays)


def back_kernel(where, own, other, *refs):
    *weights, out = refs
    core, y = where[0], where[1]
    for r, weight in enumerate(weights):
        part = contract_last(own[...], weight[core]) + contract_last(other[...], weight[1 - core])
        out[(y + len(weights) - r) % len(weights)] = part.astype(BF16)


def gate_kernel(where, parts, saved, out):
    back_grad = jnp.sum(parts[...].astype(F32), axis=0)
    pre_gate = saved[0].astype(F32)
    pre_up = saved[1].astype(F32)
    sigmoid = jax.nn.sigmoid(pre_gate)
    grad_gate = back_grad * pre_up * sigmoid * (1.0 + pre_gate * (1.0 - sigmoid))
    grad_up = back_grad * pre_gate * sigmoid
    term = jnp.sum(grad_up * pre_up, axis=1, keepdims=True)
    lane = lax.broadcasted_iota(jnp.int32, (term.shape[0], LANES), 1)
    hidden = pre_gate.shape[1]
    out[:, :hidden] = grad_gate.astype(BF16)
    out[:, hidden : 2 * hidden] = grad_up.astype(BF16)
    out[:, 2 * hidden :] = jnp.where(lane == 0, term, 0.0).astype(BF16)


def row_kernel(where, mine, theirs, own, other, out):
    core = where[0]
    ys, share = other.shape[1], other.shape[2]
    spare = out.shape[2] - share
    hidden = own.shape[2]
    row = lax.broadcasted_iota(jnp.int32, (share + spare, LANES), 0)
    lane = lax.broadcasted_iota(jnp.int32, (share + spare, LANES), 1)
    blank = jnp.zeros((spare, 2 * hidden), BF16)

    def wide(gate, up, column):
        weights = jnp.concatenate([jnp.concatenate([gate, up], axis=1), blank], axis=0)
        passing = jnp.where((row == column) & (lane == 0), 1.0, 0.0).astype(BF16)
        return jnp.concatenate([weights, passing], axis=1)

    for y in range(ys):
        at = pl.ds(pl.multiple_of((2 * y + core) * share, 16), share)
        total = contract_last(mine[...], wide(own[0, at, :], own[1, at, :], share))
        total += contract_last(theirs[...], wide(other[0, y], other[1, y], share + 1))
        out[y] = total.astype(BF16)


def pack_kernel(where, parts, out):
    total = jnp.sum(parts[...].astype(F32), axis=0)
    slots, width = total.shape
    share = SHARE
    lane = lax.broadcasted_iota(jnp.int32, (slots, width), 1)
    gates = jnp.sum(jnp.where(lane >= share, total, 0.0), axis=1, keepdims=True)
    high = gates.astype(BF16).astype(F32)
    low = gates - high
    packed = jnp.where(lane == share, high, jnp.where(lane == share + 1, low, total))
    out[...] = packed.astype(BF16).reshape(out.shape)


SHARE = 448


def per_device(
    grad_out,
    expert_ids,
    gate_values,
    w_gate_up,
    w_down,
    saved_routed,
    shared_gate_up,
    shared_down,
    saved_shared,
):
    experts = lax.axis_size(OWNER)
    xs = lax.axis_size("x")
    zs = lax.axis_size("z")
    ys = lax.axis_size("y")
    parts = lax.axis_size(PARTS)
    tokens, features = grad_out.shape
    choose = expert_ids.shape[1]
    slots = saved_routed.shape[2]
    hidden = w_down.shape[1]
    capacity = slots // experts
    share = features // parts
    wide = -(-share // LANES) * LANES
    core = lax.axis_index("core")
    y = lax.axis_index("y")
    part = lax.axis_index(PARTS)
    swap = [(0, 1), (1, 0)]
    where = jnp.stack([core, y]).astype(jnp.int32)

    piece = jnp.concatenate([shared_gate_up, shared_down.T[None]], axis=0)
    column = from_everyone(piece, "x")
    pieces = lax.all_gather(column, "z", axis=0)

    slot = jnp.arange(slots, dtype=jnp.int32)
    hit = expert_ids.T[:, None, :] == (slot // capacity)[None, :, None]
    chosen = jnp.any(hit, axis=0)
    earlier = jnp.arange(tokens)[:, None] < jnp.arange(tokens)[None, :]
    before = jnp.dot(chosen.astype(BF16), earlier.astype(BF16), preferred_element_type=F32)
    source = chosen & (before.astype(jnp.int32) == (slot % capacity)[:, None])
    columns = lax.dynamic_slice_in_dim(grad_out, part * share, share, 1)
    send = jnp.dot(source.astype(BF16), columns, preferred_element_type=F32).astype(BF16)
    send = send.reshape(experts, capacity, share)
    own_rows = exchange(send, OWNER)
    own_rows = own_rows.reshape(slots, share)

    blocks = w_down[0].reshape(hidden, ys, 2, share).transpose(1, 2, 0, 3)
    downs = []
    for r in range(ys):
        block = lax.dynamic_index_in_dim(blocks, (y + r) % ys, 0, keepdims=False)
        if r > 0:
            block = lax.ppermute(block, "y", [(i, (i + r) % ys) for i in range(ys)])
        downs.append(block)
    other_rows = lax.ppermute(own_rows, "core", swap)
    back_part = kernel_call(
        back_kernel,
        jax.ShapeDtypeStruct((ys, slots, hidden), BF16),
        where,
        own_rows,
        other_rows,
        *downs,
    )
    back_parts = exchange(back_part, "y")
    mine = kernel_call(
        gate_kernel,
        jax.ShapeDtypeStruct((slots, 3 * LANES), BF16),
        where,
        back_parts,
        saved_routed[0],
    )

    halves = w_gate_up[0].reshape(2, ys, 2, share, hidden)
    other_half = lax.ppermute(
        lax.dynamic_index_in_dim(halves, 1 - core, 2, keepdims=False), "core", swap
    )
    theirs = lax.ppermute(mine, "core", swap)
    row_part = kernel_call(
        row_kernel,
        jax.ShapeDtypeStruct((ys, slots, wide), BF16),
        where,
        mine,
        theirs,
        w_gate_up[0],
        other_half,
    )
    row_parts = exchange(row_part, "y")
    finished = kernel_call(
        pack_kernel,
        jax.ShapeDtypeStruct((experts, capacity, wide), BF16),
        where,
        row_parts,
    )
    returned = exchange(finished, OWNER)

    turned = grad_out.reshape(tokens, xs, zs, -1).transpose(0, 2, 1, 3).reshape(tokens, -1)
    down_all = pieces[:, :, 2].reshape(features, hidden)
    gate_all = pieces[:, :, 0].reshape(features, hidden)
    up_all = pieces[:, :, 1].reshape(features, hidden)
    shared_back = jnp.dot(turned, down_all, preferred_element_type=F32)
    shared_gate, shared_up = swiglu_grads(shared_back, saved_shared[0], saved_shared[1])
    shared_term = contract_last(shared_gate, gate_all) + contract_last(shared_up, up_all)
    shared_term = (
        shared_term.astype(BF16)
        .reshape(tokens, zs, xs, -1)
        .transpose(0, 2, 1, 3)
        .reshape(tokens, features)
    )
    everyone = lax.all_gather(shared_term, PARTS, axis=0)
    ours = lax.dynamic_slice_in_dim(everyone, part * share, share, 2)
    shared_sum = jnp.sum(ours.astype(F32), axis=0)

    pick = (hit & source[None]).transpose(0, 2, 1).reshape(choose * tokens, slots)
    picked = jnp.dot(
        pick.astype(BF16), returned.reshape(slots, wide), preferred_element_type=F32
    ).reshape(choose, tokens, wide)
    routed = jnp.sum(picked[:, :, :share] * gate_values.T[:, :, None], axis=0)
    grad_gates = jnp.sum(picked[:, :, share : share + 2], axis=2).T
    return (routed + shared_sum).astype(BF16), grad_gates


def solution(mesh):
    finer = Mesh(mesh.devices.reshape(4, 16, 4, 2), ("x", "z", "y", "core"))
    placed = (
        P(OWNER, None),
        P(OWNER, None),
        P(OWNER, None),
        P(OWNER, None, None, PARTS),
        P(OWNER, PARTS, None),
        P(OWNER, None, None, PARTS),
        P(None, OWNER, PARTS),
        P(PARTS, OWNER),
        P(None, OWNER, PARTS),
    )

    return jax.shard_map(
        per_device,
        mesh=finer,
        in_specs=placed,
        out_specs=(P(OWNER, PARTS), P(OWNER, None)),
        check_vma=False,
    )
```

```python
import jax
import jax.numpy as jnp
from jax import lax
from jax.experimental import pallas as pl
from jax.experimental.pallas import tpu as pltpu
from jax.sharding import Mesh
from jax.sharding import PartitionSpec as P

OWNER = ("x", "z")
PARTS = ("y", "core")
F32 = jnp.float32
BF16 = jnp.bfloat16
LANES = 128


def exchange(array, axis):
    return lax.all_to_all(array, axis, 0, 0, tiled=True)


def from_everyone(array, axis):
    peers = lax.axis_size(axis)
    return exchange(jnp.broadcast_to(array[None], (peers, *array.shape)), axis)


def contract_last(left, right):
    return lax.dot_general(left, right, (((1,), (1,)), ((), ())), preferred_element_type=F32)


def swiglu_grads(back_grad, saved_gate, saved_up):
    pre_gate = saved_gate.astype(F32)
    pre_up = saved_up.astype(F32)
    sigmoid = jax.nn.sigmoid(pre_gate)
    grad_gate = (back_grad * pre_up * sigmoid * (1.0 + pre_gate * (1.0 - sigmoid))).astype(BF16)
    grad_up = (back_grad * pre_gate * sigmoid).astype(BF16)
    return grad_gate, grad_up


def kernel_call(body, out_shape, scalars, *arrays):
    smem = pl.BlockSpec(memory_space=pltpu.SMEM)
    vmem = pl.BlockSpec(memory_space=pltpu.VMEM)
    return pl.pallas_call(
        body,
        out_shape=out_shape,
        in_specs=[smem] + [vmem] * len(arrays),
        out_specs=jax.tree.map(lambda _: vmem, out_shape),
        compiler_params=pltpu.CompilerParams(vmem_limit_bytes=10 * 2**20),
    )(scalars, *arrays)


def split_kernel(where, whole, *outs):
    y = where[1]
    _, features = whole.shape
    width = features // len(outs)
    for r, out in enumerate(outs):
        at = pl.multiple_of(((y + r) % len(outs)) * width, LANES)
        both = whole[:, pl.ds(at, width)]
        out[0] = both[:, : width // 2]
        out[1] = both[:, width // 2 :]


def back_kernel(where, own, other, *refs):
    *weights, out = refs
    core, y = where[0], where[1]
    for r, weight in enumerate(weights):
        part = contract_last(own[...], weight[core]) + contract_last(other[...], weight[1 - core])
        out[(y + len(weights) - r) % len(weights)] = part.astype(BF16)


def gate_kernel(where, parts, saved, out):
    back_grad = jnp.sum(parts[...].astype(F32), axis=0)
    pre_gate = saved[0].astype(F32)
    pre_up = saved[1].astype(F32)
    sigmoid = jax.nn.sigmoid(pre_gate)
    grad_gate = back_grad * pre_up * sigmoid * (1.0 + pre_gate * (1.0 - sigmoid))
    grad_up = back_grad * pre_gate * sigmoid
    term = jnp.sum(grad_up * pre_up, axis=1, keepdims=True)
    lane = lax.broadcasted_iota(jnp.int32, (term.shape[0], LANES), 1)
    hidden = pre_gate.shape[1]
    out[:, :hidden] = grad_gate.astype(BF16)
    out[:, hidden : 2 * hidden] = grad_up.astype(BF16)
    out[:, 2 * hidden :] = jnp.where(lane == 0, term, 0.0).astype(BF16)


def row_kernel(where, mine, theirs, own, other, out):
    core = where[0]
    ys, share = other.shape[1], other.shape[2]
    spare = out.shape[2] - share
    hidden = own.shape[2]
    row = lax.broadcasted_iota(jnp.int32, (share + spare, LANES), 0)
    lane = lax.broadcasted_iota(jnp.int32, (share + spare, LANES), 1)
    blank = jnp.zeros((spare, 2 * hidden), BF16)

    def wide(gate, up, column):
        weights = jnp.concatenate([jnp.concatenate([gate, up], axis=1), blank], axis=0)
        passing = jnp.where((row == column) & (lane == 0), 1.0, 0.0).astype(BF16)
        return jnp.concatenate([weights, passing], axis=1)

    for y in range(ys):
        at = pl.ds(pl.multiple_of((2 * y + core) * share, 16), share)
        total = contract_last(mine[...], wide(own[0, at, :], own[1, at, :], share))
        total += contract_last(theirs[...], wide(other[0, y], other[1, y], share + 1))
        out[y] = total.astype(BF16)


def pack_kernel(where, parts, out):
    total = jnp.sum(parts[...].astype(F32), axis=0)
    slots, width = total.shape
    share = SHARE
    lane = lax.broadcasted_iota(jnp.int32, (slots, width), 1)
    gates = jnp.sum(jnp.where(lane >= share, total, 0.0), axis=1, keepdims=True)
    high = gates.astype(BF16).astype(F32)
    low = gates - high
    packed = jnp.where(lane == share, high, jnp.where(lane == share + 1, low, total))
    out[...] = packed.astype(BF16).reshape(out.shape)


SHARE = 448


def per_device(
    grad_out,
    expert_ids,
    gate_values,
    w_gate_up,
    w_down,
    saved_routed,
    shared_gate_up,
    shared_down,
    saved_shared,
):
    experts = lax.axis_size(OWNER)
    xs = lax.axis_size("x")
    zs = lax.axis_size("z")
    ys = lax.axis_size("y")
    parts = lax.axis_size(PARTS)
    tokens, features = grad_out.shape
    choose = expert_ids.shape[1]
    slots = saved_routed.shape[2]
    hidden = w_down.shape[1]
    capacity = slots // experts
    share = features // parts
    wide = -(-share // LANES) * LANES
    core = lax.axis_index("core")
    y = lax.axis_index("y")
    part = lax.axis_index(PARTS)
    swap = [(0, 1), (1, 0)]
    where = jnp.stack([core, y]).astype(jnp.int32)

    piece = jnp.concatenate([shared_gate_up, shared_down.T[None]], axis=0)
    column = from_everyone(piece, "x")
    pieces = lax.all_gather(column, "z", axis=0)

    slot = jnp.arange(slots, dtype=jnp.int32)
    hit = expert_ids.T[:, None, :] == (slot // capacity)[None, :, None]
    chosen = jnp.any(hit, axis=0)
    earlier = jnp.arange(tokens)[:, None] < jnp.arange(tokens)[None, :]
    before = jnp.dot(chosen.astype(BF16), earlier.astype(BF16), preferred_element_type=F32)
    source = chosen & (before.astype(jnp.int32) == (slot % capacity)[:, None])
    columns = lax.dynamic_slice_in_dim(grad_out, part * share, share, 1)
    send = jnp.dot(source.astype(BF16), columns, preferred_element_type=F32).astype(BF16)
    send = send.reshape(experts, capacity, share)
    own_rows = exchange(send, OWNER)
    own_rows = own_rows.reshape(slots, share)

    downs = kernel_call(
        split_kernel,
        [jax.ShapeDtypeStruct((2, hidden, share), BF16)] * ys,
        where,
        w_down[0],
    )
    downs = [downs[0]] + [
        lax.ppermute(downs[r], "y", [(i, (i + r) % ys) for i in range(ys)])
        for r in range(1, ys)
    ]
    other_rows = lax.ppermute(own_rows, "core", swap)
    back_part = kernel_call(
        back_kernel,
        jax.ShapeDtypeStruct((ys, slots, hidden), BF16),
        where,
        own_rows,
        other_rows,
        *downs,
    )
    back_parts = exchange(back_part, "y")
    mine = kernel_call(
        gate_kernel,
        jax.ShapeDtypeStruct((slots, 3 * LANES), BF16),
        where,
        back_parts,
        saved_routed[0],
    )

    halves = w_gate_up[0].reshape(2, ys, 2, share, hidden)
    other_half = lax.ppermute(
        lax.dynamic_index_in_dim(halves, 1 - core, 2, keepdims=False), "core", swap
    )
    theirs = lax.ppermute(mine, "core", swap)
    row_part = kernel_call(
        row_kernel,
        jax.ShapeDtypeStruct((ys, slots, wide), BF16),
        where,
        mine,
        theirs,
        w_gate_up[0],
        other_half,
    )
    row_parts = exchange(row_part, "y")
    finished = kernel_call(
        pack_kernel,
        jax.ShapeDtypeStruct((experts, capacity, wide), BF16),
        where,
        row_parts,
    )
    returned = exchange(finished, OWNER)

    turned = grad_out.reshape(tokens, xs, zs, -1).transpose(0, 2, 1, 3).reshape(tokens, -1)
    down_all = pieces[:, :, 2].reshape(features, hidden)
    gate_all = pieces[:, :, 0].reshape(features, hidden)
    up_all = pieces[:, :, 1].reshape(features, hidden)
    shared_back = jnp.dot(turned, down_all, preferred_element_type=F32)
    shared_gate, shared_up = swiglu_grads(shared_back, saved_shared[0], saved_shared[1])
    shared_term = contract_last(shared_gate, gate_all) + contract_last(shared_up, up_all)
    shared_term = (
        shared_term.astype(BF16)
        .reshape(tokens, zs, xs, -1)
        .transpose(0, 2, 1, 3)
        .reshape(tokens, features)
    )
    everyone = lax.all_gather(shared_term, PARTS, axis=0)
    ours = lax.dynamic_slice_in_dim(everyone, part * share, share, 2)
    shared_sum = jnp.sum(ours.astype(F32), axis=0)

    pick = (hit & source[None]).transpose(0, 2, 1).reshape(choose * tokens, slots)
    picked = jnp.dot(
        pick.astype(BF16), returned.reshape(slots, wide), preferred_element_type=F32
    ).reshape(choose, tokens, wide)
    routed = jnp.sum(picked[:, :, :share] * gate_values.T[:, :, None], axis=0)
    grad_gates = jnp.sum(picked[:, :, share : share + 2], axis=2).T
    return (routed + shared_sum).astype(BF16), grad_gates


def solution(mesh):
    finer = Mesh(mesh.devices.reshape(4, 16, 4, 2), ("x", "z", "y", "core"))
    placed = (
        P(OWNER, None),
        P(OWNER, None),
        P(OWNER, None),
        P(OWNER, None, None, PARTS),
        P(OWNER, PARTS, None),
        P(OWNER, None, None, PARTS),
        P(None, OWNER, PARTS),
        P(PARTS, OWNER),
        P(None, OWNER, PARTS),
    )

    return jax.shard_map(
        per_device,
        mesh=finer,
        in_specs=placed,
        out_specs=(P(OWNER, PARTS), P(OWNER, None)),
        check_vma=False,
    )
```

```python
import jax
import jax.numpy as jnp
from jax import lax
from jax.experimental import pallas as pl
from jax.experimental.pallas import tpu as pltpu
from jax.sharding import Mesh
from jax.sharding import PartitionSpec as P

OWNER = ("x", "z")
PARTS = ("y", "core")
F32 = jnp.float32
BF16 = jnp.bfloat16
LANES = 128


def exchange(array, axis):
    return lax.all_to_all(array, axis, 0, 0, tiled=True)


def contract_last(left, right):
    return lax.dot_general(left, right, (((1,), (1,)), ((), ())), preferred_element_type=F32)


def swiglu_grads(back_grad, saved_gate, saved_up):
    pre_gate = saved_gate.astype(F32)
    pre_up = saved_up.astype(F32)
    sigmoid = jax.nn.sigmoid(pre_gate)
    grad_gate = (back_grad * pre_up * sigmoid * (1.0 + pre_gate * (1.0 - sigmoid))).astype(BF16)
    grad_up = (back_grad * pre_gate * sigmoid).astype(BF16)
    return grad_gate, grad_up


def kernel_call(body, out_shape, scalars, *arrays):
    smem = pl.BlockSpec(memory_space=pltpu.SMEM)
    vmem = pl.BlockSpec(memory_space=pltpu.VMEM)
    return pl.pallas_call(
        body,
        out_shape=out_shape,
        in_specs=[smem] + [vmem] * len(arrays),
        out_specs=jax.tree.map(lambda _: vmem, out_shape),
        compiler_params=pltpu.CompilerParams(vmem_limit_bytes=10 * 2**20),
    )(scalars, *arrays)


def spread_kernel(where, pair, last, out):
    for peer in range(out.shape[0]):
        out[peer, :2] = pair[...]
        out[peer, 2] = last[...]


def route_kernel(where, ids, tokens, out):
    core, y = where[0], where[1]
    experts, half, width = out.shape
    count = tokens.shape[0]
    shape = (experts * half, count)
    row = lax.broadcasted_iota(jnp.int32, shape, 0)
    expert = row // half
    chosen = ids[0:1, :] == expert
    for k in range(1, ids.shape[0]):
        chosen = chosen | (ids[k : k + 1, :] == expert)
    chosen = jnp.where(chosen, 1.0, 0.0)
    first = lax.broadcasted_iota(jnp.int32, (count, count), 0)
    second = lax.broadcasted_iota(jnp.int32, (count, count), 1)
    earlier = jnp.where(first < second, 1.0, 0.0).astype(BF16)
    before = jnp.dot(chosen.astype(BF16), earlier, preferred_element_type=F32)
    place = (row % half + half * core).astype(F32)
    source = jnp.where(before == place, chosen, 0.0).astype(BF16)
    columns = tokens[:, pl.ds(pl.multiple_of(y * width, LANES), width)]
    rows = jnp.dot(source, columns, preferred_element_type=F32).astype(BF16)
    out[...] = rows.reshape(out.shape)


def shared_kernel(where, turned, pieces, saved, out):
    count = pieces.shape[0]
    back_grad = jnp.zeros(saved.shape[1:], F32)
    for z in range(count):
        back_grad += jnp.dot(turned[z], pieces[z, 2], preferred_element_type=F32)
    grads = jnp.concatenate(swiglu_grads(back_grad, saved[0], saved[1]), axis=1)
    for z in range(count):
        weights = jnp.concatenate([pieces[z, 0], pieces[z, 1]], axis=1)
        out[z] = contract_last(grads, weights).astype(BF16)


def split_kernel(where, whole, *outs):
    y = where[1]
    width = whole.shape[1] // len(outs)
    for r, out in enumerate(outs):
        at = pl.multiple_of(((y + r) % len(outs)) * width, LANES)
        out[...] = whole[:, pl.ds(at, width)]


def back_kernel(where, arrived, own, other, out):
    y = where[1]
    ys, hidden = own.shape[:2]
    rows = arrived[...].reshape(out.shape[1], own.shape[2])
    for r in range(ys):
        home = (y + ys - r) % ys
        out[home, :, :hidden] = contract_last(rows, own[r]).astype(BF16)
        out[home, :, hidden:] = contract_last(rows, other[r]).astype(BF16)


def gate_kernel(where, parts, own, other, grads, gates):
    core = where[0]
    back_grad = jnp.sum(parts[...].astype(F32), axis=0)
    rows, width = back_grad.shape
    slots = own.shape[1]
    row = lax.broadcasted_iota(jnp.int32, (rows, slots), 0)
    slot = lax.broadcasted_iota(jnp.int32, (rows, slots), 1)
    take = jnp.where(slot == (row // 2) * 4 + row % 2 + 2 * core, 1.0, 0.0).astype(BF16)

    def saved(g):
        mine = jnp.dot(take, own[g], preferred_element_type=F32)
        theirs = jnp.dot(take, other[g], preferred_element_type=F32)
        return jnp.concatenate([mine, theirs], axis=1)

    pre_gate, pre_up = saved(0), saved(1)
    sigmoid = jax.nn.sigmoid(pre_gate)
    grad_gate = back_grad * pre_up * sigmoid * (1.0 + pre_gate * (1.0 - sigmoid))
    grad_up = back_grad * pre_gate * sigmoid
    term = jnp.sum(grad_up * pre_up, axis=1, keepdims=True)
    grads[:, :width] = grad_gate.astype(BF16)
    grads[:, width:] = grad_up.astype(BF16)
    gates[...] = jnp.broadcast_to(term, (rows, rows)).T.astype(BF16)


def row_kernel(where, grads, gates, own, other, out):
    ys, width = out.shape[0], out.shape[2]
    rows = grads.shape[0]
    extra = out.shape[1] - rows
    for y in range(ys):
        at = slice(y * width, (y + 1) * width)
        weights = jnp.concatenate(
            [own[0, at, :], other[0, at, :], own[1, at, :], other[1, at, :]], axis=1
        )
        out[y, :rows, :] = contract_last(grads[...], weights).astype(BF16)
        out[y, rows:, :rows] = gates[:extra, :]
        out[y, rows:, rows:] = jnp.zeros((extra, width - rows), BF16)


def pack_kernel(where, parts, out):
    rows = out.shape[0] * out.shape[1]
    total = jnp.sum(parts[...].astype(F32), axis=0)
    gates = jnp.broadcast_to(total[rows : rows + 1, :rows], (rows, rows)).T
    high = gates.astype(BF16).astype(F32)
    lane = lax.broadcasted_iota(jnp.int32, (rows, rows), 1)
    spare = jnp.where(lane == 0, high, jnp.where(lane == 1, gates - high, 0.0))
    packed = jnp.concatenate([total[:rows], spare], axis=1)
    out[...] = packed.astype(BF16).reshape(out.shape)


def pick_kernel(where, ids, gate_values, returned, keep, give):
    core = where[0]
    count, choose = ids.shape
    half = returned.shape[1]
    rows = returned.shape[0] * half
    share = (returned.shape[2] - LANES) // 2
    row = lax.broadcasted_iota(jnp.int32, (count, rows), 1)
    expert = row // half
    hits = [jnp.where(ids[:, k : k + 1] == expert, 1.0, 0.0) for k in range(choose)]
    chosen = sum(hits[1:], hits[0])
    first = lax.broadcasted_iota(jnp.int32, (count, count), 1)
    second = lax.broadcasted_iota(jnp.int32, (count, count), 0)
    earlier = jnp.where(first < second, 1.0, 0.0).astype(BF16)
    before = jnp.dot(earlier, chosen.astype(BF16), preferred_element_type=F32)
    place = (row % half + half * core).astype(F32)
    source = jnp.where(before == place, chosen, 0.0)
    weight = sum(hits[k] * gate_values[:, k : k + 1] for k in range(choose)) * source
    high = weight.astype(BF16)
    low = (weight - high.astype(F32)).astype(BF16)
    values = returned[...].reshape(rows, returned.shape[2])
    routed = jnp.dot(high, values, preferred_element_type=F32)
    routed += jnp.dot(low, values, preferred_element_type=F32)
    tail = values[:, 2 * share :].astype(F32)
    gates = jnp.broadcast_to(tail[:, 0:1] + tail[:, 1:2], (rows, rows)).T[0:1, :]
    lane = lax.broadcasted_iota(jnp.int32, (count, LANES), 1)
    spare = jnp.zeros((count, LANES), F32)
    for k in range(choose):
        term = jnp.sum(hits[k] * source * gates, axis=1, keepdims=True)
        spare = jnp.where(lane == k, term, spare)
    left, right = routed[:, :share], routed[:, share : 2 * share]
    keep[:, :share] = jnp.where(core == 0, left, right)
    give[:, :share] = jnp.where(core == 0, right, left)
    keep[:, share:] = spare[:, : keep.shape[1] - share]
    give[:, share:] = spare[:, : keep.shape[1] - share]


def per_device(
    grad_out,
    expert_ids,
    gate_values,
    w_gate_up,
    w_down,
    saved_routed,
    shared_gate_up,
    shared_down,
    saved_shared,
):
    experts = lax.axis_size(OWNER)
    xs = lax.axis_size("x")
    zs = lax.axis_size("z")
    ys = lax.axis_size("y")
    parts = lax.axis_size(PARTS)
    tokens, features = grad_out.shape
    choose = expert_ids.shape[1]
    slots = saved_routed.shape[2]
    hidden = w_down.shape[1]
    capacity = slots // experts
    share = features // parts
    core = lax.axis_index("core")
    y = lax.axis_index("y")
    part = lax.axis_index(PARTS)
    swap = [(0, 1), (1, 0)]
    where = jnp.stack([core, y]).astype(jnp.int32)
    half = capacity // 2
    width = 2 * share
    rows = experts * half

    spread = kernel_call(
        spread_kernel,
        jax.ShapeDtypeStruct((xs, 3, *shared_gate_up.shape[1:]), BF16),
        where,
        shared_gate_up,
        shared_down.T,
    )
    column = exchange(spread, "x")
    column = column.transpose(1, 0, 2, 3).reshape(3, -1, hidden)
    pieces = lax.all_gather(column, "z", axis=0)

    send = kernel_call(
        route_kernel,
        jax.ShapeDtypeStruct((experts, half, width), BF16),
        where,
        expert_ids.T,
        grad_out,
    )
    arrived = exchange(send, OWNER)

    downs = kernel_call(
        split_kernel,
        [jax.ShapeDtypeStruct((hidden, width), BF16)] * ys,
        where,
        w_down[0],
    )
    downs = [downs[0]] + [
        lax.ppermute(downs[r], "y", [(i, (i + r) % ys) for i in range(ys)])
        for r in range(1, ys)
    ]
    own_down = jnp.stack(downs)
    other_down = lax.ppermute(own_down, "core", swap)
    other_saved = lax.ppermute(saved_routed[0], "core", swap)
    other_gate_up = lax.ppermute(w_gate_up[0], "core", swap)

    back_part = kernel_call(
        back_kernel,
        jax.ShapeDtypeStruct((ys, rows, 2 * hidden), BF16),
        where,
        arrived,
        own_down,
        other_down,
    )
    back_parts = exchange(back_part, "y")
    grads, gates = kernel_call(
        gate_kernel,
        [
            jax.ShapeDtypeStruct((rows, 4 * hidden), BF16),
            jax.ShapeDtypeStruct((rows, rows), BF16),
        ],
        where,
        back_parts,
        saved_routed[0],
        other_saved,
    )
    row_part = kernel_call(
        row_kernel,
        jax.ShapeDtypeStruct((ys, rows + 8, width), BF16),
        where,
        grads,
        gates,
        w_gate_up[0],
        other_gate_up,
    )
    row_parts = exchange(row_part, "y")
    finished = kernel_call(
        pack_kernel,
        jax.ShapeDtypeStruct((experts, half, width + LANES), BF16),
        where,
        row_parts,
    )
    returned = exchange(finished, OWNER)

    turned = grad_out.reshape(tokens, xs, zs, -1).transpose(2, 0, 1, 3)
    turned = turned.reshape(zs, tokens, -1)
    shared_term = kernel_call(
        shared_kernel,
        jax.ShapeDtypeStruct((zs, tokens, features // zs), BF16),
        where,
        turned,
        pieces,
        saved_shared,
    )
    shared_term = shared_term.reshape(zs, tokens, xs, -1).transpose(1, 2, 0, 3)
    shared_term = shared_term.reshape(tokens, features)
    everyone = lax.all_gather(shared_term, PARTS, axis=0)
    ours = lax.dynamic_slice_in_dim(everyone, part * share, share, 2)
    shared_sum = jnp.sum(ours.astype(F32), axis=0)

    keep, give = kernel_call(
        pick_kernel,
        [jax.ShapeDtypeStruct((tokens, share + 64), F32)] * 2,
        where,
        expert_ids,
        gate_values,
        returned,
    )
    taken = lax.ppermute(give, "core", swap)
    total = keep + taken
    grad_in = (total[:, :share] + shared_sum).astype(BF16)
    return grad_in, total[:, share : share + choose]


def solution(mesh):
    finer = Mesh(mesh.devices.reshape(4, 16, 4, 2), ("x", "z", "y", "core"))
    placed = (
        P(OWNER, None),
        P(OWNER, None),
        P(OWNER, None),
        P(OWNER, None, None, PARTS),
        P(OWNER, PARTS, None),
        P(OWNER, None, None, PARTS),
        P(None, OWNER, PARTS),
        P(PARTS, OWNER),
        P(None, OWNER, PARTS),
    )

    return jax.shard_map(
        per_device,
        mesh=finer,
        in_specs=placed,
        out_specs=(P(OWNER, PARTS), P(OWNER, None)),
        check_vma=False,
    )
```

```python
import jax
import jax.numpy as jnp
from jax import lax
from jax.experimental import pallas as pl
from jax.experimental.pallas import tpu as pltpu
from jax.sharding import Mesh
from jax.sharding import PartitionSpec as P

OWNER = ("x", "z")
PARTS = ("y", "core")
F32 = jnp.float32
BF16 = jnp.bfloat16
LANES = 128


def exchange(array, axis):
    return lax.all_to_all(array, axis, 0, 0, tiled=True)


def contract_last(left, right):
    return lax.dot_general(left, right, (((1,), (1,)), ((), ())), preferred_element_type=F32)


def swiglu_grads(back_grad, saved_gate, saved_up):
    pre_gate = saved_gate.astype(F32)
    pre_up = saved_up.astype(F32)
    sigmoid = jax.nn.sigmoid(pre_gate)
    grad_gate = (back_grad * pre_up * sigmoid * (1.0 + pre_gate * (1.0 - sigmoid))).astype(BF16)
    grad_up = (back_grad * pre_gate * sigmoid).astype(BF16)
    return grad_gate, grad_up


def kernel_call(body, out_shape, scalars, *arrays):
    smem = pl.BlockSpec(memory_space=pltpu.SMEM)
    vmem = pl.BlockSpec(memory_space=pltpu.VMEM)
    return pl.pallas_call(
        body,
        out_shape=out_shape,
        in_specs=[smem] + [vmem] * len(arrays),
        out_specs=jax.tree.map(lambda _: vmem, out_shape),
        compiler_params=pltpu.CompilerParams(vmem_limit_bytes=10 * 2**20),
    )(scalars, *arrays)


def route_kernel(where, ids, tokens, out):
    core, y = where[0], where[1]
    experts, capacity, share = out.shape
    count = tokens.shape[0]
    shape = (experts * capacity, count)
    slot = lax.broadcasted_iota(jnp.int32, shape, 0)
    expert = slot // capacity
    chosen = ids[0:1, :] == expert
    for k in range(1, ids.shape[0]):
        chosen = chosen | (ids[k : k + 1, :] == expert)
    chosen = jnp.where(chosen, 1.0, 0.0)
    first = lax.broadcasted_iota(jnp.int32, (count, count), 0)
    second = lax.broadcasted_iota(jnp.int32, (count, count), 1)
    earlier = jnp.where(first < second, 1.0, 0.0).astype(BF16)
    before = jnp.dot(chosen.astype(BF16), earlier, preferred_element_type=F32)
    place = (slot % capacity).astype(F32)
    source = jnp.where(before == place, chosen, 0.0).astype(BF16)
    both = tokens[:, pl.ds(pl.multiple_of(y * 2 * share, LANES), 2 * share)]
    columns = jnp.where(core == 0, both[:, :share], both[:, share:])
    rows = jnp.dot(source, columns, preferred_element_type=F32).astype(BF16)
    out[...] = rows.reshape(out.shape)


def shared_kernel(where, turned, pieces, saved, mine, theirs, terms):
    core = where[0]
    count, half = pieces.shape[0], mine.shape[0]
    back_grad = jnp.zeros(saved.shape[1:], F32)
    for z in range(count):
        back_grad += jnp.dot(turned[z], pieces[z, 2], preferred_element_type=F32)
    grads = jnp.concatenate(swiglu_grads(back_grad, saved[0], saved[1]), axis=1)
    for z in range(count):
        weights = jnp.concatenate([pieces[z, 0], pieces[z, 1]], axis=1)
        terms[z] = contract_last(grads, weights).astype(BF16)
    mine[...] = terms[pl.ds(half * core, half)]
    theirs[...] = terms[pl.ds(half * (1 - core), half)]


def fold_kernel(where, mine, taken, *outs):
    y = where[1]
    count = mine.shape[0]
    ys = len(outs)
    piece = mine.shape[2] // ys
    for z in range(count):
        total = (mine[z].astype(F32) + taken[z].astype(F32)).astype(BF16)
        parts = [total[:, x * piece : (x + 1) * piece] for x in range(ys)]
        for r, out in enumerate(outs):
            home = (y + r) % ys
            chosen = parts[ys - 1]
            for x in range(ys - 1):
                chosen = jnp.where(home == x, parts[x], chosen)
            out[:, z * piece : (z + 1) * piece] = chosen


def split_kernel(where, whole, *outs):
    y = where[1]
    _, features = whole.shape
    width = features // len(outs)
    for r, out in enumerate(outs):
        at = pl.multiple_of(((y + r) % len(outs)) * width, LANES)
        both = whole[:, pl.ds(at, width)]
        out[0] = both[:, : width // 2]
        out[1] = both[:, width // 2 :]


def back_kernel(where, own, other, *refs):
    *weights, out = refs
    core, y = where[0], where[1]
    mine = own[...].reshape(out.shape[1], own.shape[2])
    theirs = other[...].reshape(mine.shape)
    for r, weight in enumerate(weights):
        part = contract_last(mine, weight[core]) + contract_last(theirs, weight[1 - core])
        out[(y + len(weights) - r) % len(weights)] = part.astype(BF16)


def gate_kernel(where, parts, saved, out):
    back_grad = jnp.sum(parts[...].astype(F32), axis=0)
    pre_gate = saved[0].astype(F32)
    pre_up = saved[1].astype(F32)
    sigmoid = jax.nn.sigmoid(pre_gate)
    grad_gate = back_grad * pre_up * sigmoid * (1.0 + pre_gate * (1.0 - sigmoid))
    grad_up = back_grad * pre_gate * sigmoid
    term = jnp.sum(grad_up * pre_up, axis=1, keepdims=True)
    lane = lax.broadcasted_iota(jnp.int32, (term.shape[0], LANES), 1)
    hidden = pre_gate.shape[1]
    out[:, :hidden] = grad_gate.astype(BF16)
    out[:, hidden : 2 * hidden] = grad_up.astype(BF16)
    out[:, 2 * hidden :] = jnp.where(lane == 0, term, 0.0).astype(BF16)


def row_kernel(where, mine, theirs, own, other, out):
    core = where[0]
    ys, share = other.shape[1], other.shape[2]
    spare = out.shape[2] - share
    hidden = own.shape[2]
    row = lax.broadcasted_iota(jnp.int32, (share + spare, LANES), 0)
    lane = lax.broadcasted_iota(jnp.int32, (share + spare, LANES), 1)
    blank = jnp.zeros((spare, 2 * hidden), BF16)

    def wide(gate, up, column):
        weights = jnp.concatenate([jnp.concatenate([gate, up], axis=1), blank], axis=0)
        passing = jnp.where((row == column) & (lane == 0), 1.0, 0.0).astype(BF16)
        return jnp.concatenate([weights, passing], axis=1)

    for y in range(ys):
        at = pl.ds(pl.multiple_of((2 * y + core) * share, 16), share)
        total = contract_last(mine[...], wide(own[0, at, :], own[1, at, :], share))
        total += contract_last(theirs[...], wide(other[0, y], other[1, y], share + 1))
        out[y] = total.astype(BF16)


def pack_kernel(where, parts, out):
    total = jnp.sum(parts[...].astype(F32), axis=0)
    slots, width = total.shape
    share = SHARE
    lane = lax.broadcasted_iota(jnp.int32, (slots, width), 1)
    gates = jnp.sum(jnp.where(lane >= share, total, 0.0), axis=1, keepdims=True)
    high = gates.astype(BF16).astype(F32)
    low = gates - high
    packed = jnp.where(lane == share, high, jnp.where(lane == share + 1, low, total))
    out[...] = packed.astype(BF16).reshape(out.shape)


SHARE = 448


def per_device(
    grad_out,
    expert_ids,
    gate_values,
    w_gate_up,
    w_down,
    saved_routed,
    shared_gate_up,
    shared_down,
    saved_shared,
):
    experts = lax.axis_size(OWNER)
    xs = lax.axis_size("x")
    zs = lax.axis_size("z")
    ys = lax.axis_size("y")
    parts = lax.axis_size(PARTS)
    tokens, features = grad_out.shape
    choose = expert_ids.shape[1]
    slots = saved_routed.shape[2]
    hidden = w_down.shape[1]
    capacity = slots // experts
    share = features // parts
    wide = -(-share // LANES) * LANES
    core = lax.axis_index("core")
    y = lax.axis_index("y")
    swap = [(0, 1), (1, 0)]
    where = jnp.stack([core, y]).astype(jnp.int32)

    piece = jnp.concatenate([shared_gate_up, shared_down.T[None]], axis=0)
    column = exchange(jnp.broadcast_to(piece[None], (xs, *piece.shape)), "x")
    column = column.transpose(1, 0, 2, 3).reshape(3, -1, hidden)
    pieces = lax.all_gather(column, "z", axis=0)

    send = kernel_call(
        route_kernel,
        jax.ShapeDtypeStruct((experts, capacity, share), BF16),
        where,
        expert_ids.T,
        grad_out,
    )
    own_rows = exchange(send, OWNER)

    downs = kernel_call(
        split_kernel,
        [jax.ShapeDtypeStruct((2, hidden, share), BF16)] * ys,
        where,
        w_down[0],
    )
    downs = [downs[0]] + [
        lax.ppermute(downs[r], "y", [(i, (i + r) % ys) for i in range(ys)])
        for r in range(1, ys)
    ]
    other_rows = lax.ppermute(own_rows, "core", swap)
    back_part = kernel_call(
        back_kernel,
        jax.ShapeDtypeStruct((ys, slots, hidden), BF16),
        where,
        own_rows,
        other_rows,
        *downs,
    )
    back_parts = exchange(back_part, "y")
    mine = kernel_call(
        gate_kernel,
        jax.ShapeDtypeStruct((slots, 3 * LANES), BF16),
        where,
        back_parts,
        saved_routed[0],
    )

    halves = w_gate_up[0].reshape(2, ys, 2, share, hidden)
    other_half = lax.ppermute(
        lax.dynamic_index_in_dim(halves, 1 - core, 2, keepdims=False), "core", swap
    )
    theirs = lax.ppermute(mine, "core", swap)
    row_part = kernel_call(
        row_kernel,
        jax.ShapeDtypeStruct((ys, slots, wide), BF16),
        where,
        mine,
        theirs,
        w_gate_up[0],
        other_half,
    )
    row_parts = exchange(row_part, "y")
    finished = kernel_call(
        pack_kernel,
        jax.ShapeDtypeStruct((experts, capacity, wide), BF16),
        where,
        row_parts,
    )
    returned = exchange(finished, OWNER)

    turned = grad_out.reshape(tokens, xs, zs, -1).transpose(2, 0, 1, 3)
    turned = turned.reshape(zs, tokens, -1)
    half = jax.ShapeDtypeStruct((zs // 2, tokens, features // zs), BF16)
    shared_mine, shared_theirs = pl.pallas_call(
        shared_kernel,
        out_shape=[half, half],
        in_specs=[pl.BlockSpec(memory_space=pltpu.SMEM)]
        + [pl.BlockSpec(memory_space=pltpu.VMEM)] * 3,
        out_specs=[pl.BlockSpec(memory_space=pltpu.VMEM)] * 2,
        scratch_shapes=[pltpu.VMEM((zs, *half.shape[1:]), BF16)],
        compiler_params=pltpu.CompilerParams(vmem_limit_bytes=10 * 2**20),
    )(where, turned, pieces, saved_shared)
    shared_taken = lax.ppermute(shared_theirs, "core", swap)
    folded = kernel_call(
        fold_kernel,
        [jax.ShapeDtypeStruct((tokens, share), BF16)] * ys,
        where,
        shared_mine,
        shared_taken,
    )
    folded = [folded[0]] + [
        lax.ppermute(folded[r], "y", [(i, (i + r) % ys) for i in range(ys)])
        for r in range(1, ys)
    ]
    shared_sum = sum(block.astype(F32) for block in folded)

    slot = jnp.arange(slots, dtype=jnp.int32)
    hit = expert_ids.T[:, None, :] == (slot // capacity)[None, :, None]
    chosen = jnp.any(hit, axis=0)
    earlier = jnp.arange(tokens)[:, None] < jnp.arange(tokens)[None, :]
    before = jnp.dot(chosen.astype(BF16), earlier.astype(BF16), preferred_element_type=F32)
    source = chosen & (before.astype(jnp.int32) == (slot % capacity)[:, None])
    pick = (hit & source[None]).transpose(0, 2, 1).reshape(choose * tokens, slots)
    picked = jnp.dot(
        pick.astype(BF16), returned.reshape(slots, wide), preferred_element_type=F32
    ).reshape(choose, tokens, wide)
    routed = jnp.sum(picked[:, :, :share] * gate_values.T[:, :, None], axis=0)
    grad_gates = jnp.sum(picked[:, :, share : share + 2], axis=2).T
    return (routed + shared_sum).astype(BF16), grad_gates


def solution(mesh):
    finer = Mesh(mesh.devices.reshape(4, 16, 4, 2), ("x", "z", "y", "core"))
    placed = (
        P(OWNER, None),
        P(OWNER, None),
        P(OWNER, None),
        P(OWNER, None, None, PARTS),
        P(OWNER, PARTS, None),
        P(OWNER, None, None, PARTS),
        P(None, OWNER, PARTS),
        P(PARTS, OWNER),
        P(None, OWNER, PARTS),
    )

    return jax.shard_map(
        per_device,
        mesh=finer,
        in_specs=placed,
        out_specs=(P(OWNER, PARTS), P(OWNER, None)),
        check_vma=False,
    )
```

```python
import jax
import jax.numpy as jnp
from jax import lax
from jax.experimental import pallas as pl
from jax.experimental.pallas import tpu as pltpu
from jax.sharding import Mesh
from jax.sharding import PartitionSpec as P

OWNER = ("x", "z")
PARTS = ("y", "core")
F32 = jnp.float32
BF16 = jnp.bfloat16
LANES = 128


def exchange(array, axis):
    return lax.all_to_all(array, axis, 0, 0, tiled=True)


def contract_last(left, right):
    return lax.dot_general(left, right, (((1,), (1,)), ((), ())), preferred_element_type=F32)


def swiglu_grads(back_grad, saved_gate, saved_up):
    pre_gate = saved_gate.astype(F32)
    pre_up = saved_up.astype(F32)
    sigmoid = jax.nn.sigmoid(pre_gate)
    grad_gate = (back_grad * pre_up * sigmoid * (1.0 + pre_gate * (1.0 - sigmoid))).astype(BF16)
    grad_up = (back_grad * pre_gate * sigmoid).astype(BF16)
    return grad_gate, grad_up


def kernel_call(body, out_shape, scalars, *arrays):
    smem = pl.BlockSpec(memory_space=pltpu.SMEM)
    vmem = pl.BlockSpec(memory_space=pltpu.VMEM)
    return pl.pallas_call(
        body,
        out_shape=out_shape,
        in_specs=[smem] + [vmem] * len(arrays),
        out_specs=jax.tree.map(lambda _: vmem, out_shape),
        compiler_params=pltpu.CompilerParams(vmem_limit_bytes=10 * 2**20),
    )(scalars, *arrays)


def route_kernel(where, ids, tokens, out):
    core, y = where[0], where[1]
    experts, capacity, share = out.shape
    count = tokens.shape[0]
    shape = (experts * capacity, count)
    slot = lax.broadcasted_iota(jnp.int32, shape, 0)
    expert = slot // capacity
    chosen = ids[0:1, :] == expert
    for k in range(1, ids.shape[0]):
        chosen = chosen | (ids[k : k + 1, :] == expert)
    chosen = jnp.where(chosen, 1.0, 0.0)
    first = lax.broadcasted_iota(jnp.int32, (count, count), 0)
    second = lax.broadcasted_iota(jnp.int32, (count, count), 1)
    earlier = jnp.where(first < second, 1.0, 0.0).astype(BF16)
    before = jnp.dot(chosen.astype(BF16), earlier, preferred_element_type=F32)
    place = (slot % capacity).astype(F32)
    source = jnp.where(before == place, chosen, 0.0).astype(BF16)
    both = tokens[:, pl.ds(pl.multiple_of(y * 2 * share, LANES), 2 * share)]
    columns = jnp.where(core == 0, both[:, :share], both[:, share:])
    rows = jnp.dot(source, columns, preferred_element_type=F32).astype(BF16)
    out[...] = rows.reshape(out.shape)


def shared_kernel(where, turned, pieces, saved, mine, theirs, terms):
    core = where[0]
    count, half = pieces.shape[0], mine.shape[0]
    back_grad = jnp.zeros(saved.shape[1:], F32)
    for z in range(count):
        back_grad += jnp.dot(turned[z], pieces[z, 2], preferred_element_type=F32)
    grads = jnp.concatenate(swiglu_grads(back_grad, saved[0], saved[1]), axis=1)
    for z in range(count):
        weights = jnp.concatenate([pieces[z, 0], pieces[z, 1]], axis=1)
        terms[z] = contract_last(grads, weights).astype(BF16)
    mine[...] = terms[pl.ds(half * core, half)]
    theirs[...] = terms[pl.ds(half * (1 - core), half)]


def fold_kernel(where, mine, taken, *outs):
    y = where[1]
    count = mine.shape[0]
    ys = len(outs)
    piece = mine.shape[2] // ys
    for z in range(count):
        total = (mine[z].astype(F32) + taken[z].astype(F32)).astype(BF16)
        parts = [total[:, x * piece : (x + 1) * piece] for x in range(ys)]
        for r, out in enumerate(outs):
            home = (y + r) % ys
            chosen = parts[ys - 1]
            for x in range(ys - 1):
                chosen = jnp.where(home == x, parts[x], chosen)
            out[:, z * piece : (z + 1) * piece] = chosen


def split_kernel(where, whole, *outs):
    y = where[1]
    _, features = whole.shape
    width = features // len(outs)
    for r, out in enumerate(outs):
        at = pl.multiple_of(((y + r) % len(outs)) * width, LANES)
        both = whole[:, pl.ds(at, width)]
        out[0] = both[:, : width // 2]
        out[1] = both[:, width // 2 :]


def back_kernel(where, own, other, *refs):
    *weights, out = refs
    core, y = where[0], where[1]
    mine = own[...].reshape(out.shape[1], own.shape[2])
    theirs = other[...].reshape(mine.shape)
    for r, weight in enumerate(weights):
        part = contract_last(mine, weight[core]) + contract_last(theirs, weight[1 - core])
        out[(y + len(weights) - r) % len(weights)] = part.astype(BF16)


def gate_kernel(where, parts, saved, out):
    back_grad = jnp.sum(parts[...].astype(F32), axis=0)
    pre_gate = saved[0].astype(F32)
    pre_up = saved[1].astype(F32)
    sigmoid = jax.nn.sigmoid(pre_gate)
    grad_gate = back_grad * pre_up * sigmoid * (1.0 + pre_gate * (1.0 - sigmoid))
    grad_up = back_grad * pre_gate * sigmoid
    term = jnp.sum(grad_up * pre_up, axis=1, keepdims=True)
    lane = lax.broadcasted_iota(jnp.int32, (term.shape[0], LANES), 1)
    hidden = pre_gate.shape[1]
    out[:, :hidden] = grad_gate.astype(BF16)
    out[:, hidden : 2 * hidden] = grad_up.astype(BF16)
    out[:, 2 * hidden :] = jnp.where(lane == 0, term, 0.0).astype(BF16)


def row_kernel(where, mine, theirs, own, other, out):
    core = where[0]
    ys, share = other.shape[1], other.shape[2]
    slots = mine.shape[0]
    half = slots // 2
    width = 2 * own.shape[2]
    cut = share // LANES * LANES
    blank = jnp.zeros((LANES - share % LANES, width), BF16)

    def turned(grads):
        column = grads[:, width : width + 1].astype(F32)
        return jnp.broadcast_to(column, (slots, LANES)).T[0:8, :]

    row = lax.broadcasted_iota(jnp.int32, (8, slots), 0)
    gates = jnp.where(row == 0, turned(mine), jnp.where(row == 1, turned(theirs), 0.0))
    for y in range(ys):
        at = pl.ds(pl.multiple_of((2 * y + core) * share, 16), share)
        ours = jnp.concatenate([own[0, at, :], own[1, at, :]], axis=1)
        others = jnp.concatenate([other[0, y], other[1, y]], axis=1)

        def block(rows, before, after):
            left = contract_last(mine[rows, :width], jnp.concatenate(before + [ours] + after, 0))
            right = jnp.concatenate(before + [others] + after, 0)
            return left + contract_last(theirs[rows, :width], right)

        first = block(slice(0, half), [], [blank])
        second = block(slice(half, slots), [blank], [])
        out[y, :half, :cut] = first[:, :cut].astype(BF16)
        out[y, :half, cut : cut + LANES] = (first[:, cut:] + second[:, :LANES]).astype(BF16)
        out[y, :half, cut + LANES :] = second[:, LANES:].astype(BF16)
        out[y, half:, :slots] = gates.astype(BF16)
        out[y, half:, slots:] = jnp.zeros((8, out.shape[2] - slots), BF16)


def pack_kernel(where, parts, out):
    total = jnp.sum(parts[...].astype(F32), axis=0)
    wide = out.shape[2]
    half = out.shape[0] * out.shape[1] // 2
    share = total.shape[1] // 2
    terms = total[half : half + 1, : 2 * half] + total[half + 1 : half + 2, : 2 * half]
    gates = jnp.broadcast_to(terms, (LANES, 2 * half)).T[:, 0:1]
    high = gates.astype(BF16).astype(F32)
    first = total[:half, :wide]
    second = pltpu.roll(total[:half, 2 * share - wide :], share, 1)
    rows = jnp.concatenate([first, second], axis=0)
    lane = lax.broadcasted_iota(jnp.int32, rows.shape, 1)
    spare = jnp.where(lane == share, high, jnp.where(lane == share + 1, gates - high, 0.0))
    packed = jnp.where(lane < share, rows, spare)
    out[...] = packed.astype(BF16).reshape(out.shape)


def per_device(
    grad_out,
    expert_ids,
    gate_values,
    w_gate_up,
    w_down,
    saved_routed,
    shared_gate_up,
    shared_down,
    saved_shared,
):
    experts = lax.axis_size(OWNER)
    xs = lax.axis_size("x")
    zs = lax.axis_size("z")
    ys = lax.axis_size("y")
    parts = lax.axis_size(PARTS)
    tokens, features = grad_out.shape
    choose = expert_ids.shape[1]
    slots = saved_routed.shape[2]
    hidden = w_down.shape[1]
    capacity = slots // experts
    share = features // parts
    wide = -(-share // LANES) * LANES
    core = lax.axis_index("core")
    y = lax.axis_index("y")
    swap = [(0, 1), (1, 0)]
    where = jnp.stack([core, y]).astype(jnp.int32)

    piece = jnp.concatenate([shared_gate_up, shared_down.T[None]], axis=0)
    column = exchange(jnp.broadcast_to(piece[None], (xs, *piece.shape)), "x")
    column = column.transpose(1, 0, 2, 3).reshape(3, -1, hidden)
    pieces = lax.all_gather(column, "z", axis=0)

    send = kernel_call(
        route_kernel,
        jax.ShapeDtypeStruct((experts, capacity, share), BF16),
        where,
        expert_ids.T,
        grad_out,
    )
    own_rows = exchange(send, OWNER)

    downs = kernel_call(
        split_kernel,
        [jax.ShapeDtypeStruct((2, hidden, share), BF16)] * ys,
        where,
        w_down[0],
    )
    downs = [downs[0]] + [
        lax.ppermute(downs[r], "y", [(i, (i + r) % ys) for i in range(ys)])
        for r in range(1, ys)
    ]
    other_rows = lax.ppermute(own_rows, "core", swap)
    back_part = kernel_call(
        back_kernel,
        jax.ShapeDtypeStruct((ys, slots, hidden), BF16),
        where,
        own_rows,
        other_rows,
        *downs,
    )
    back_parts = exchange(back_part, "y")
    mine = kernel_call(
        gate_kernel,
        jax.ShapeDtypeStruct((slots, 3 * LANES), BF16),
        where,
        back_parts,
        saved_routed[0],
    )

    halves = w_gate_up[0].reshape(2, ys, 2, share, hidden)
    other_half = lax.ppermute(
        lax.dynamic_index_in_dim(halves, 1 - core, 2, keepdims=False), "core", swap
    )
    theirs = lax.ppermute(mine, "core", swap)
    row_part = kernel_call(
        row_kernel,
        jax.ShapeDtypeStruct((ys, slots // 2 + 8, 2 * share), BF16),
        where,
        mine,
        theirs,
        w_gate_up[0],
        other_half,
    )
    row_parts = exchange(row_part, "y")
    finished = kernel_call(
        pack_kernel,
        jax.ShapeDtypeStruct((experts, capacity, wide), BF16),
        where,
        row_parts,
    )
    returned = exchange(finished, OWNER)

    turned = grad_out.reshape(tokens, xs, zs, -1).transpose(2, 0, 1, 3)
    turned = turned.reshape(zs, tokens, -1)
    half = jax.ShapeDtypeStruct((zs // 2, tokens, features // zs), BF16)
    shared_mine, shared_theirs = pl.pallas_call(
        shared_kernel,
        out_shape=[half, half],
        in_specs=[pl.BlockSpec(memory_space=pltpu.SMEM)]
        + [pl.BlockSpec(memory_space=pltpu.VMEM)] * 3,
        out_specs=[pl.BlockSpec(memory_space=pltpu.VMEM)] * 2,
        scratch_shapes=[pltpu.VMEM((zs, *half.shape[1:]), BF16)],
        compiler_params=pltpu.CompilerParams(vmem_limit_bytes=10 * 2**20),
    )(where, turned, pieces, saved_shared)
    shared_taken = lax.ppermute(shared_theirs, "core", swap)
    folded = kernel_call(
        fold_kernel,
        [jax.ShapeDtypeStruct((tokens, share), BF16)] * ys,
        where,
        shared_mine,
        shared_taken,
    )
    folded = [folded[0]] + [
        lax.ppermute(folded[r], "y", [(i, (i + r) % ys) for i in range(ys)])
        for r in range(1, ys)
    ]
    shared_sum = sum(block.astype(F32) for block in folded)

    slot = jnp.arange(slots, dtype=jnp.int32)
    hit = expert_ids.T[:, None, :] == (slot // capacity)[None, :, None]
    chosen = jnp.any(hit, axis=0)
    earlier = jnp.arange(tokens)[:, None] < jnp.arange(tokens)[None, :]
    before = jnp.dot(chosen.astype(BF16), earlier.astype(BF16), preferred_element_type=F32)
    source = chosen & (before.astype(jnp.int32) == (slot % capacity)[:, None])
    pick = (hit & source[None]).transpose(0, 2, 1).reshape(choose * tokens, slots)
    picked = jnp.dot(
        pick.astype(BF16), returned.reshape(slots, wide), preferred_element_type=F32
    ).reshape(choose, tokens, wide)
    routed = jnp.sum(picked[:, :, :share] * gate_values.T[:, :, None], axis=0)
    grad_gates = jnp.sum(picked[:, :, share : share + 2], axis=2).T
    return (routed + shared_sum).astype(BF16), grad_gates


def solution(mesh):
    finer = Mesh(mesh.devices.reshape(4, 16, 4, 2), ("x", "z", "y", "core"))
    placed = (
        P(OWNER, None),
        P(OWNER, None),
        P(OWNER, None),
        P(OWNER, None, None, PARTS),
        P(OWNER, PARTS, None),
        P(OWNER, None, None, PARTS),
        P(None, OWNER, PARTS),
        P(PARTS, OWNER),
        P(None, OWNER, PARTS),
    )

    return jax.shard_map(
        per_device,
        mesh=finer,
        in_specs=placed,
        out_specs=(P(OWNER, PARTS), P(OWNER, None)),
        check_vma=False,
    )
```

```python
import jax
import jax.numpy as jnp
from jax import lax
from jax.experimental import pallas as pl
from jax.experimental.pallas import tpu as pltpu
from jax.sharding import Mesh
from jax.sharding import PartitionSpec as P

OWNER = ("x", "z")
PARTS = ("y", "core")
F32 = jnp.float32
BF16 = jnp.bfloat16
LANES = 128


def exchange(array, axis):
    return lax.all_to_all(array, axis, 0, 0, tiled=True)


def contract_last(left, right):
    return lax.dot_general(left, right, (((1,), (1,)), ((), ())), preferred_element_type=F32)


def swiglu_grads(back_grad, saved_gate, saved_up):
    pre_gate = saved_gate.astype(F32)
    pre_up = saved_up.astype(F32)
    sigmoid = jax.nn.sigmoid(pre_gate)
    grad_gate = (back_grad * pre_up * sigmoid * (1.0 + pre_gate * (1.0 - sigmoid))).astype(BF16)
    grad_up = (back_grad * pre_gate * sigmoid).astype(BF16)
    return grad_gate, grad_up


def kernel_call(body, out_shape, scalars, *arrays):
    smem = pl.BlockSpec(memory_space=pltpu.SMEM)
    vmem = pl.BlockSpec(memory_space=pltpu.VMEM)
    return pl.pallas_call(
        body,
        out_shape=out_shape,
        in_specs=[smem] + [vmem] * len(arrays),
        out_specs=jax.tree.map(lambda _: vmem, out_shape),
        compiler_params=pltpu.CompilerParams(vmem_limit_bytes=10 * 2**20),
    )(scalars, *arrays)


def route_kernel(where, ids, tokens, out):
    core, y = where[0], where[1]
    experts, capacity, share = out.shape
    count = tokens.shape[0]
    shape = (experts * capacity, count)
    slot = lax.broadcasted_iota(jnp.int32, shape, 0)
    expert = slot // capacity
    chosen = ids[0:1, :] == expert
    for k in range(1, ids.shape[0]):
        chosen = chosen | (ids[k : k + 1, :] == expert)
    chosen = jnp.where(chosen, 1.0, 0.0)
    first = lax.broadcasted_iota(jnp.int32, (count, count), 0)
    second = lax.broadcasted_iota(jnp.int32, (count, count), 1)
    earlier = jnp.where(first < second, 1.0, 0.0).astype(BF16)
    before = jnp.dot(chosen.astype(BF16), earlier, preferred_element_type=F32)
    place = (slot % capacity).astype(F32)
    source = jnp.where(before == place, chosen, 0.0).astype(BF16)
    both = tokens[:, pl.ds(pl.multiple_of(y * 2 * share, LANES), 2 * share)]
    columns = jnp.where(core == 0, both[:, :share], both[:, share:])
    rows = jnp.dot(source, columns, preferred_element_type=F32).astype(BF16)
    out[...] = rows.reshape(out.shape)


def shared_kernel(where, turned, pieces, saved, mine, theirs, terms):
    core = where[0]
    count, half = pieces.shape[0], mine.shape[0]
    back_grad = jnp.zeros(saved.shape[1:], F32)
    for z in range(count):
        back_grad += jnp.dot(turned[z], pieces[z, 2], preferred_element_type=F32)
    grads = jnp.concatenate(swiglu_grads(back_grad, saved[0], saved[1]), axis=1)
    for z in range(count):
        weights = jnp.concatenate([pieces[z, 0], pieces[z, 1]], axis=1)
        terms[z] = contract_last(grads, weights).astype(BF16)
    mine[...] = terms[pl.ds(half * core, half)]
    theirs[...] = terms[pl.ds(half * (1 - core), half)]


def fold_kernel(where, mine, taken, *outs):
    y = where[1]
    count = mine.shape[0]
    ys = len(outs)
    piece = mine.shape[2] // ys
    for z in range(count):
        total = (mine[z].astype(F32) + taken[z].astype(F32)).astype(BF16)
        parts = [total[:, x * piece : (x + 1) * piece] for x in range(ys)]
        for r, out in enumerate(outs):
            home = (y + r) % ys
            chosen = parts[ys - 1]
            for x in range(ys - 1):
                chosen = jnp.where(home == x, parts[x], chosen)
            out[:, z * piece : (z + 1) * piece] = chosen


def split_kernel(where, whole, *outs):
    y = where[1]
    _, features = whole.shape
    width = features // len(outs)
    for r, out in enumerate(outs):
        at = pl.multiple_of(((y + r) % len(outs)) * width, LANES)
        both = whole[:, pl.ds(at, width)]
        out[0] = both[:, : width // 2]
        out[1] = both[:, width // 2 :]


def back_kernel(where, own, other, *refs):
    *weights, out = refs
    core, y = where[0], where[1]
    mine = own[...].reshape(out.shape[1], own.shape[2])
    theirs = other[...].reshape(mine.shape)
    count, hidden = len(weights), out.shape[2]
    for r in range(0, count, 2):
        pair = weights[r : r + 2]
        part = contract_last(mine, jnp.concatenate([w[core] for w in pair], axis=0))
        part += contract_last(theirs, jnp.concatenate([w[1 - core] for w in pair], axis=0))
        for i in range(2):
            block = part[:, i * hidden : (i + 1) * hidden]
            out[(y + count - r - i) % count] = block.astype(BF16)


def gate_kernel(where, parts, saved, out):
    back_grad = jnp.sum(parts[...].astype(F32), axis=0)
    pre_gate = saved[0].astype(F32)
    pre_up = saved[1].astype(F32)
    sigmoid = jax.nn.sigmoid(pre_gate)
    grad_gate = back_grad * pre_up * sigmoid * (1.0 + pre_gate * (1.0 - sigmoid))
    grad_up = back_grad * pre_gate * sigmoid
    term = jnp.sum(grad_up * pre_up, axis=1, keepdims=True)
    lane = lax.broadcasted_iota(jnp.int32, (term.shape[0], LANES), 1)
    hidden = pre_gate.shape[1]
    out[:, :hidden] = grad_gate.astype(BF16)
    out[:, hidden : 2 * hidden] = grad_up.astype(BF16)
    out[:, 2 * hidden :] = jnp.where(lane == 0, term, 0.0).astype(BF16)


def row_kernel(where, mine, theirs, own, other, out):
    core = where[0]
    ys, share = other.shape[1], other.shape[2]
    slots = mine.shape[0]
    half = slots // 2
    width = 2 * own.shape[2]
    cut = share // LANES * LANES
    blank = jnp.zeros((LANES - share % LANES, width), BF16)

    def turned(grads):
        column = grads[:, width : width + 1].astype(F32)
        return jnp.broadcast_to(column, (slots, LANES)).T[0:8, :]

    row = lax.broadcasted_iota(jnp.int32, (8, slots), 0)
    gates = jnp.where(row == 0, turned(mine), jnp.where(row == 1, turned(theirs), 0.0))
    for y in range(ys):
        at = pl.ds(pl.multiple_of((2 * y + core) * share, 16), share)
        ours = jnp.concatenate([own[0, at, :], own[1, at, :]], axis=1)
        others = jnp.concatenate([other[0, y], other[1, y]], axis=1)

        def block(rows, before, after):
            left = contract_last(mine[rows, :width], jnp.concatenate(before + [ours] + after, 0))
            right = jnp.concatenate(before + [others] + after, 0)
            return left + contract_last(theirs[rows, :width], right)

        first = block(slice(0, half), [], [blank])
        second = block(slice(half, slots), [blank], [])
        out[y, :half, :cut] = first[:, :cut].astype(BF16)
        out[y, :half, cut : cut + LANES] = (first[:, cut:] + second[:, :LANES]).astype(BF16)
        out[y, :half, cut + LANES :] = second[:, LANES:].astype(BF16)
        out[y, half:, :slots] = gates.astype(BF16)
        out[y, half:, slots:] = jnp.zeros((8, out.shape[2] - slots), BF16)


def pack_kernel(where, parts, out):
    total = jnp.sum(parts[...].astype(F32), axis=0)
    wide = out.shape[2]
    half = out.shape[0] * out.shape[1] // 2
    share = total.shape[1] // 2
    terms = total[half : half + 1, : 2 * half] + total[half + 1 : half + 2, : 2 * half]
    gates = jnp.broadcast_to(terms, (LANES, 2 * half)).T[:, 0:1]
    high = gates.astype(BF16).astype(F32)
    first = total[:half, :wide]
    second = pltpu.roll(total[:half, 2 * share - wide :], share, 1)
    rows = jnp.concatenate([first, second], axis=0)
    lane = lax.broadcasted_iota(jnp.int32, rows.shape, 1)
    spare = jnp.where(lane == share, high, jnp.where(lane == share + 1, gates - high, 0.0))
    packed = jnp.where(lane < share, rows, spare)
    out[...] = packed.astype(BF16).reshape(out.shape)


def per_device(
    grad_out,
    expert_ids,
    gate_values,
    w_gate_up,
    w_down,
    saved_routed,
    shared_gate_up,
    shared_down,
    saved_shared,
):
    experts = lax.axis_size(OWNER)
    xs = lax.axis_size("x")
    zs = lax.axis_size("z")
    ys = lax.axis_size("y")
    parts = lax.axis_size(PARTS)
    tokens, features = grad_out.shape
    choose = expert_ids.shape[1]
    slots = saved_routed.shape[2]
    hidden = w_down.shape[1]
    capacity = slots // experts
    share = features // parts
    wide = -(-share // LANES) * LANES
    core = lax.axis_index("core")
    y = lax.axis_index("y")
    swap = [(0, 1), (1, 0)]
    where = jnp.stack([core, y]).astype(jnp.int32)

    piece = jnp.concatenate([shared_gate_up, shared_down.T[None]], axis=0)
    column = exchange(jnp.broadcast_to(piece[None], (xs, *piece.shape)), "x")
    column = column.transpose(1, 0, 2, 3).reshape(3, -1, hidden)
    pieces = lax.all_gather(column, "z", axis=0)

    send = kernel_call(
        route_kernel,
        jax.ShapeDtypeStruct((experts, capacity, share), BF16),
        where,
        expert_ids.T,
        grad_out,
    )
    own_rows = exchange(send, OWNER)

    downs = kernel_call(
        split_kernel,
        [jax.ShapeDtypeStruct((2, hidden, share), BF16)] * ys,
        where,
        w_down[0],
    )
    downs = [downs[0]] + [
        lax.ppermute(downs[r], "y", [(i, (i + r) % ys) for i in range(ys)])
        for r in range(1, ys)
    ]
    other_rows = lax.ppermute(own_rows, "core", swap)
    back_part = kernel_call(
        back_kernel,
        jax.ShapeDtypeStruct((ys, slots, hidden), BF16),
        where,
        own_rows,
        other_rows,
        *downs,
    )
    back_parts = exchange(back_part, "y")
    mine = kernel_call(
        gate_kernel,
        jax.ShapeDtypeStruct((slots, 3 * LANES), BF16),
        where,
        back_parts,
        saved_routed[0],
    )

    halves = w_gate_up[0].reshape(2, ys, 2, share, hidden)
    other_half = lax.ppermute(
        lax.dynamic_index_in_dim(halves, 1 - core, 2, keepdims=False), "core", swap
    )
    theirs = lax.ppermute(mine, "core", swap)
    row_part = kernel_call(
        row_kernel,
        jax.ShapeDtypeStruct((ys, slots // 2 + 8, 2 * share), BF16),
        where,
        mine,
        theirs,
        w_gate_up[0],
        other_half,
    )
    row_parts = exchange(row_part, "y")
    finished = kernel_call(
        pack_kernel,
        jax.ShapeDtypeStruct((experts, capacity, wide), BF16),
        where,
        row_parts,
    )
    returned = exchange(finished, OWNER)

    turned = grad_out.reshape(tokens, xs, zs, -1).transpose(2, 0, 1, 3)
    turned = turned.reshape(zs, tokens, -1)
    half = jax.ShapeDtypeStruct((zs // 2, tokens, features // zs), BF16)
    shared_mine, shared_theirs = pl.pallas_call(
        shared_kernel,
        out_shape=[half, half],
        in_specs=[pl.BlockSpec(memory_space=pltpu.SMEM)]
        + [pl.BlockSpec(memory_space=pltpu.VMEM)] * 3,
        out_specs=[pl.BlockSpec(memory_space=pltpu.VMEM)] * 2,
        scratch_shapes=[pltpu.VMEM((zs, *half.shape[1:]), BF16)],
        compiler_params=pltpu.CompilerParams(vmem_limit_bytes=10 * 2**20),
    )(where, turned, pieces, saved_shared)
    shared_taken = lax.ppermute(shared_theirs, "core", swap)
    folded = kernel_call(
        fold_kernel,
        [jax.ShapeDtypeStruct((tokens, share), BF16)] * ys,
        where,
        shared_mine,
        shared_taken,
    )
    folded = [folded[0]] + [
        lax.ppermute(folded[r], "y", [(i, (i + r) % ys) for i in range(ys)])
        for r in range(1, ys)
    ]
    shared_sum = sum(block.astype(F32) for block in folded)

    slot = jnp.arange(slots, dtype=jnp.int32)
    hit = expert_ids.T[:, None, :] == (slot // capacity)[None, :, None]
    chosen = jnp.any(hit, axis=0)
    earlier = jnp.arange(tokens)[:, None] < jnp.arange(tokens)[None, :]
    before = jnp.dot(chosen.astype(BF16), earlier.astype(BF16), preferred_element_type=F32)
    source = chosen & (before.astype(jnp.int32) == (slot % capacity)[:, None])
    pick = (hit & source[None]).transpose(0, 2, 1).reshape(choose * tokens, slots)
    picked = jnp.dot(
        pick.astype(BF16), returned.reshape(slots, wide), preferred_element_type=F32
    ).reshape(choose, tokens, wide)
    routed = jnp.sum(picked[:, :, :share] * gate_values.T[:, :, None], axis=0)
    grad_gates = jnp.sum(picked[:, :, share : share + 2], axis=2).T
    return (routed + shared_sum).astype(BF16), grad_gates


def solution(mesh):
    finer = Mesh(mesh.devices.reshape(4, 16, 4, 2), ("x", "z", "y", "core"))
    placed = (
        P(OWNER, None),
        P(OWNER, None),
        P(OWNER, None),
        P(OWNER, None, None, PARTS),
        P(OWNER, PARTS, None),
        P(OWNER, None, None, PARTS),
        P(None, OWNER, PARTS),
        P(PARTS, OWNER),
        P(None, OWNER, PARTS),
    )

    return jax.shard_map(
        per_device,
        mesh=finer,
        in_specs=placed,
        out_specs=(P(OWNER, PARTS), P(OWNER, None)),
        check_vma=False,
    )
```
